32 devices in a mesh: dp: 2 (over y), row: 4 (over x, core), col: 4 (over z).
Axes of the slice: x: 2, y: 2, z: 4, core: 2. Of those that a mesh axis runs over, the one named last changes fastest.
Arguments:
- tokens: bfloat16 [2048, 8192], P(('dp', 'col'), 'row'), may hold values from -6 to 6
- frozen_weight: bfloat16 [8192, 8192], P('row', 'col'), may hold values from -0.0625 to 0.0625
- input_adapter_factor: bfloat16 [16, 8192], P(None, 'row'), may hold values from -0.0625 to 0.0625
- output_adapter_factor: bfloat16 [16, 8192], P(None, 'col'), may hold values from -1.5 to 1.5
- magnitude: float32 [8192], P('col'), may hold values from 0.5 to 2
- cotangent: bfloat16 [2048, 8192], P(('dp', 'row'), 'col'), may hold values from -6 to 6
- sequence_lengths: int32 [2, 8], P('dp'), may hold values from 1 to 512, 1024 in all within a row
Outputs:
- projected: bfloat16 [2048, 8192], P(('dp', 'row'), 'col')
- grad_mag: float32 [8192], P('col')
- input_factor_gradient: float32 [16, 8192], P(None, 'row')
- grad_b: float32 [16, 8192], P(None, 'col')
The draws below stay inside these ranges and needn't reach their ends.
Inputs may be any that keep to these rules, and one draw needn't show every extreme that they name: `sequence_lengths`: each group's 8 lengths sum to 1024, and one of them is exactly 512.
All inputs are finite; a program needn't handle non-finite values.
Results may differ from the reference program's by a relative error of at most 0.0052.
Values may be sent and summed in bfloat16 or wider, within the bound.
A program may use at most 64 MiB of HBM per device.

```python
import math
import jax
import jax.numpy as jnp
import numpy as np
from jax import lax

MODEL_WIDTH = 8192
ADAPTER_RANK = 16
TOK = 1024
SEQS = 8
LONGEST = 512
GROUPS = 2
TOKENS = 2048


def levels(stream_key, dims, cuts, least, largest):
    gain = 1.0
    for position, parts in cuts:
        heights = jax.random.uniform(jax.random.fold_in(jax.random.fold_in(stream_key, 6), position), (parts,), jnp.float32, least / len(cuts), largest / len(cuts))
        gain = gain * jnp.repeat(jnp.exp(heights), dims[position] // parts).reshape((-1,) + (1,) * (len(dims) - 1 - position))
    return gain


def length_profile(count, total, reach, lean):
    weights = [(1 << 20) // math.isqrt(rank ** lean) + 1 for rank in range(2, count + 1)]
    rest, holding = total - reach - (count - 1), [1] * (count - 1)
    while rest > 0:
        free = [i for i in range(count - 1) if holding[i] < reach]
        mass, left = sum([weights[i] for i in free]), rest
        for i in free:
            extra = min(reach - holding[i], max(1, left * weights[i] // mass), rest)
            holding[i] = holding[i] + extra
            rest = rest - extra
    return np.array([reach] + holding)


def uneven(rng, amount, total, limit, skew):
    if amount == 2:
        one = jax.random.randint(rng, (), max(1, total - limit), min(limit, total - 1) + 1)
        return jnp.stack([one, total - one])
    sizes = jnp.asarray(length_profile(amount, total, limit, skew), jnp.int32)
    couples = (amount - 1) // 2
    donor, sink = sizes[1:1 + 2 * couples:2], sizes[2:2 + 2 * couples:2]
    slack = jnp.minimum(donor - 1, limit - sink)
    shifted = jax.random.randint(jax.random.fold_in(rng, 1), (couples,), 0, 1 << 20) % (slack + 1)
    sizes = sizes.at[1:1 + 2 * couples:2].set(donor - shifted).at[2:2 + 2 * couples:2].set(sink + shifted)
    return sizes[jax.random.permutation(jax.random.fold_in(rng, 2), amount)]


def centred(own_key, shape, deviation, bound, pieces=(), held_as=jnp.bfloat16):
    gain = levels(own_key, shape, pieces, -0.22, 0.18) if pieces else 1.0
    result = jax.random.normal(own_key, shape, jnp.float32) * deviation * gain
    return jnp.minimum(jnp.maximum(result, -bound), bound).astype(held_as)


def setup_inputs(seed: int = 0) -> dict:
    keys = jax.random.split(jax.random.key(seed), 8)
    tokens = centred(keys[0], (TOKENS, MODEL_WIDTH), 1.0, 6.0, ((0, 8), (1, 4)))
    frozen_weight = centred(keys[1], (MODEL_WIDTH, MODEL_WIDTH), MODEL_WIDTH ** -0.5, 0.0625, ((0, 4), (1, 4)))
    input_adapter_factor = centred(keys[2], (ADAPTER_RANK, MODEL_WIDTH), MODEL_WIDTH ** -0.5, 0.0625, ((1, 4),))
    output_adapter_factor = centred(keys[3], (ADAPTER_RANK, MODEL_WIDTH), ADAPTER_RANK ** -0.5, 1.5, ((1, 4),))
    magnitude = jnp.clip(jnp.exp(math.log(2.0) - 1.3862944 * jax.random.uniform(keys[4], (MODEL_WIDTH,), jnp.float32) ** levels(keys[4], (MODEL_WIDTH,), ((0, 4),), -0.2, 0.2)), 0.5, 2.0)
    cotangent = centred(keys[5], (TOKENS, MODEL_WIDTH), 1.0, 6.0, ((0, 8), (1, 4)))
    sequence_lengths = jax.vmap(lambda own: uneven(own, SEQS, TOK, LONGEST, 2))(jax.random.split(keys[6], GROUPS)).reshape((GROUPS, SEQS)).astype(jnp.int32)
    return dict(tokens=tokens, frozen_weight=frozen_weight, input_adapter_factor=input_adapter_factor, output_adapter_factor=output_adapter_factor, magnitude=magnitude, cotangent=cotangent, sequence_lengths=sequence_lengths)


norm_eps = 1e-06
highest_precision = lax.Precision.HIGHEST

def contract_product(left, right, left_dim, right_dim):
    return lax.dot_general(left, right, (((left_dim,), (right_dim,)), ((), ())), preferred_element_type=jnp.float32)

def token_weights(lengths, positions):
    ends = jnp.cumsum(lengths, dtype=jnp.int32)
    starts = ends - lengths
    inside = (positions[:, None] >= starts[None, :]) & (positions[:, None] < ends[None, :])
    inverse = 1.0 / lengths.astype(jnp.float32)
    return lax.optimization_barrier(jnp.sum(jnp.where(inside, inverse[None, :], jnp.float32(0.0)), axis=1))

def reference(tokens, frozen_weight, input_adapter_factor, output_adapter_factor, magnitude, cotangent, sequence_lengths):
    low_rank_update = contract_product(input_adapter_factor, output_adapter_factor, 0, 0)
    merged = frozen_weight.astype(jnp.float32) + low_rank_update
    col_norm = jnp.sqrt(lax.optimization_barrier(jnp.sum(merged * merged, axis=0)) + norm_eps)
    col_scale = magnitude / col_norm
    down_activations = contract_product(tokens, input_adapter_factor, 1, 1).astype(jnp.bfloat16)
    query_projection = jnp.dot(tokens, frozen_weight, preferred_element_type=jnp.float32) + jnp.dot(down_activations, output_adapter_factor, preferred_element_type=jnp.float32)
    projected = (query_projection * col_scale[None, :]).astype(jnp.bfloat16)
    positions = jnp.arange(TOK, dtype=jnp.int32)
    weights = jax.vmap(lambda lengths: token_weights(lengths, positions))(sequence_lengths).reshape(-1)
    grad_out = cotangent.astype(jnp.float32) * weights[:, None]
    scale_grad = lax.optimization_barrier(jnp.sum(grad_out * query_projection, axis=0))
    grad_mag = scale_grad / col_norm
    norm_coefficient = -scale_grad * magnitude / (col_norm * col_norm * col_norm)
    projection_gradient = (grad_out * col_scale[None, :]).astype(jnp.bfloat16)
    gram_product_matrix = contract_product(input_adapter_factor, input_adapter_factor, 1, 1)
    merged_input_factor = jnp.dot(input_adapter_factor, frozen_weight, preferred_element_type=jnp.float32) + jnp.dot(gram_product_matrix, output_adapter_factor.astype(jnp.float32), precision=highest_precision)
    grad_b = contract_product(down_activations, projection_gradient, 0, 0) + merged_input_factor * norm_coefficient[None, :]
    backward_rows = contract_product(projection_gradient, output_adapter_factor, 1, 1).astype(jnp.bfloat16)
    scaled_output_factor = (output_adapter_factor.astype(jnp.float32) * norm_coefficient[None, :]).astype(jnp.bfloat16)
    input_factor_gradient = contract_product(backward_rows, tokens, 0, 0) + contract_product(scaled_output_factor, frozen_weight, 1, 1)
    input_factor_gradient = input_factor_gradient + jnp.dot(contract_product(scaled_output_factor, output_adapter_factor, 1, 1), input_adapter_factor.astype(jnp.float32), precision=highest_precision)
    return (projected, grad_mag, input_factor_gradient, grad_b)
```

```python
import functools

import jax
import jax.numpy as jnp
from jax import lax
from jax.experimental import pallas as pl
from jax.experimental.pallas import tpu as pltpu
from jax.sharding import PartitionSpec as P

norm_eps = 1e-06
highest_precision = lax.Precision.HIGHEST
MESH = pl.DeviceIdType.MESH
LANES = 128
VMEM_LIMIT = 60 * 1024 * 1024


def contract_product(left, right, left_dim, right_dim):
    return lax.dot_general(
        left, right, (((left_dim,), (right_dim,)), ((), ())), preferred_element_type=jnp.float32
    )


def column_tiles(width, tile):
    return [(start, min(tile, width - start)) for start in range(0, width, tile)]


def project_kernel(
    C, R, S,
    tok, w_hbm, at_hbm, a_ref, b_ref,
    q_out, g_out, stat_out,
    wx, gath, sb, pin, xin, pb, st_mine, st_in,
    load_sem, gsend, grecv, ssend, precv, xrecv, stsend, strecv,
):
    z = lax.axis_index("col")
    r = lax.axis_index("row")
    p, q = r // 2, r % 2
    pairs = R // 2
    sub, features = tok.shape[1], tok.shape[2]
    cols = w_hbm.shape[1]
    rank_rows = a_ref.shape[0]
    units = C * S
    block_units = units // R
    tiles = column_tiles(cols, 512)

    load_w = pltpu.make_async_copy(w_hbm, wx.at[:, pl.ds(0, cols)], load_sem.at[0])
    load_a = pltpu.make_async_copy(at_hbm, wx.at[:, pl.ds(cols, LANES)], load_sem.at[1])
    load_w.start()
    load_a.start()

    barrier = pltpu.get_barrier_semaphore()

    @pl.when(z > 0)
    def _():
        pl.semaphore_signal(barrier, inc=1, device_id={"col": z - 1}, device_id_type=MESH)

    @pl.when(z < C - 1)
    def _():
        pl.semaphore_signal(barrier, inc=1, device_id={"col": z + 1}, device_id_type=MESH)

    for i in range(1, R):
        pl.semaphore_signal(barrier, inc=1, device_id={"row": (r + i) % R}, device_id_type=MESH)

    @pl.when((z > 0) & (z < C - 1))
    def _():
        pl.semaphore_wait(barrier, R + 1)

    @pl.when((z == 0) | (z == C - 1))
    def _():
        pl.semaphore_wait(barrier, R)

    def hop(src, u, direction):
        target = z - 1 if direction == 0 else z + 1
        return pltpu.make_async_remote_copy(
            src_ref=src, dst_ref=gath.at[u], send_sem=gsend.at[direction, u],
            recv_sem=grecv.at[u], device_id={"col": target}, device_id_type=MESH,
        )

    for s in range(S):
        @pl.when(z > 0)
        def _():
            hop(tok.at[s], z * S + s, 0).start()

        @pl.when(z < C - 1)
        def _():
            hop(tok.at[s], z * S + s, 1).start()

    load_w.wait()
    load_a.wait()

    st_mine[...] = jnp.zeros_like(st_mine)
    a = a_ref[...]
    gram = contract_product(a, a, 1, 1)
    for start, width in tiles:
        span = pl.ds(start, width)
        st_mine[0:rank_rows, span] = jnp.dot(
            a, wx[:, span], preferred_element_type=jnp.float32
        ) + jnp.dot(
            gram, b_ref[0:rank_rows, span].astype(jnp.float32),
            precision=highest_precision, preferred_element_type=jnp.float32,
        )
    depth = 256

    def norm_step(i, carry):
        rows = pl.ds(pl.multiple_of(i * depth, depth), depth)
        for start, width in tiles:
            span = pl.ds(start, width)
            merged = wx[rows, span].astype(jnp.float32) + jnp.dot(
                wx[rows, pl.ds(cols, LANES)], b_ref[:, span], preferred_element_type=jnp.float32
            )
            st_mine[rank_rows:rank_rows + 1, span] += jnp.sum(merged * merged, axis=0, keepdims=True)
        return carry

    lax.fori_loop(0, features // depth, norm_step, 0)

    def stat_copy(i):
        return pltpu.make_async_remote_copy(
            src_ref=st_mine, dst_ref=st_in.at[i], send_sem=stsend.at[i], recv_sem=strecv.at[i],
            device_id={"row": (r + i) % R}, device_id_type=MESH,
        )

    near = jnp.minimum(z, C - 1 - z)

    def place(k):
        j = k - S
        both = j < 2 * near * S
        rest = j - 2 * near * S
        distance = jnp.where(both, j // (2 * S) + 1, near + 1 + rest // S)
        s = jnp.where(both, (j % (2 * S)) // 2, rest % S)
        leftward = jnp.where(both, j % 2 == 0, z > C - 1 - z)
        chunk = jnp.where(leftward, z - distance, z + distance)
        own = k < S
        return jnp.where(own, z, chunk), jnp.where(own, k, s)

    def pair_copy(u):
        return pltpu.make_async_remote_copy(
            src_ref=sb.at[u], dst_ref=pin.at[u], send_sem=ssend.at[u], recv_sem=precv.at[u],
            device_id={"row": p * 2 + (1 - q)}, device_id_type=MESH,
        )

    def far_copy(u, owner_pair):
        return pltpu.make_async_remote_copy(
            src_ref=sb.at[u], dst_ref=xin.at[p, u % block_units], send_sem=ssend.at[u],
            recv_sem=xrecv.at[p, u % block_units],
            device_id={"row": owner_pair * 2 + q}, device_id_type=MESH,
        )

    def multiply(k):
        c, s = place(k)
        u = c * S + s
        owner = u // block_units

        @pl.when(k < S)
        def _():
            gath[u] = tok[s]

        @pl.when(k >= S)
        def _():
            hop(gath.at[u], u, 0).wait_recv()

            @pl.when((c < z) & (z < C - 1))
            def _():
                hop(gath.at[u], u, 1).start()

            @pl.when((c > z) & (z > 0))
            def _():
                hop(gath.at[u], u, 0).start()

        slot = k % 2
        for start, width in column_tiles(cols + LANES, 512):
            span = pl.ds(start, width)
            pb[slot, :, span] = jnp.dot(gath[u], wx[:, span], preferred_element_type=jnp.float32)

        @pl.when(owner % 2 != q)
        def _():
            sb[u] = pb[slot].astype(jnp.bfloat16)
            pair_copy(u).start()

    def combine(k):
        c, s = place(k)
        u = c * S + s
        owner = u // block_units
        slot = k % 2

        @pl.when(owner % 2 == q)
        def _():
            pair_copy(u).wait_recv()
            total = pb[slot] + pin[u].astype(jnp.float32)

            @pl.when(owner // 2 == p)
            def _():
                q_out[u % block_units] = total

            @pl.when(owner // 2 != p)
            def _():
                sb[u] = total.astype(jnp.bfloat16)
                far_copy(u, owner // 2).start()

    def step(k, carry):
        @pl.when(k < units)
        def _():
            multiply(k)

        @pl.when(k == 0)
        def _():
            for i in range(1, R):
                stat_copy(i).start()

        @pl.when(k > 0)
        def _():
            combine(k - 1)

        return carry

    lax.fori_loop(0, units + 1, step, 0)

    keep = pltpu.make_async_copy(gath, g_out, load_sem.at[0])
    keep.start()
    for i in range(1, R):
        stat_copy(i).wait_recv()
    total = st_mine[...]
    for i in range(1, R):
        total = total + st_in[i]
    stat_out[...] = total

    def finish(v, carry):
        for i in range(1, pairs):
            other = (p + i) % pairs
            pltpu.make_async_remote_copy(
                src_ref=sb.at[v], dst_ref=xin.at[other, v], send_sem=ssend.at[v],
                recv_sem=xrecv.at[other, v], device_id={"row": other * 2 + q}, device_id_type=MESH,
            ).wait_recv()
            q_out[v] += xin[other, v].astype(jnp.float32)
        return carry

    lax.fori_loop(0, block_units, finish, 0)

    for i in range(1, R):
        stat_copy(i).wait_send()

    def drain(u, carry):
        c = u // S
        owner = u // block_units

        @pl.when((owner % 2 != q) | (owner // 2 != p))
        def _():
            pair_copy(u).wait_send()

        @pl.when((c <= z) & (z < C - 1))
        def _():
            hop(gath.at[u], u, 1).wait_send()

        @pl.when((c >= z) & (z > 0))
        def _():
            hop(gath.at[u], u, 0).wait_send()

        return carry

    lax.fori_loop(0, units, drain, 0)
    keep.wait()


def gather_project(tokens, frozen_weight, input_factor, output_factor):
    C, R = lax.axis_size("col"), lax.axis_size("row")
    local_rows, features = tokens.shape
    cols = frozen_weight.shape[1]
    rank_rows = input_factor.shape[0]
    S = 4
    sub = local_rows // S
    units = C * S
    block_units = units // R
    wide = cols + LANES
    stat_rows = rank_rows + 8
    at = jnp.pad(input_factor.T, ((0, 0), (0, LANES - rank_rows)))
    bp = jnp.pad(output_factor, ((0, LANES - rank_rows), (0, 0)))
    vmem = pl.BlockSpec(memory_space=pltpu.VMEM)
    hbm = pl.BlockSpec(memory_space=pl.ANY)
    dma = pltpu.SemaphoreType.DMA
    f32, bf16 = jnp.float32, jnp.bfloat16
    return pl.pallas_call(
        functools.partial(project_kernel, C, R, S),
        out_shape=(
            jax.ShapeDtypeStruct((block_units, sub, wide), f32),
            jax.ShapeDtypeStruct((units, sub, features), bf16),
            jax.ShapeDtypeStruct((stat_rows, cols), f32),
        ),
        in_specs=[vmem, hbm, hbm, vmem, vmem],
        out_specs=(vmem, hbm, vmem),
        scratch_shapes=[
            pltpu.VMEM((features, wide), bf16),
            pltpu.VMEM((units, sub, features), bf16),
            pltpu.VMEM((units, sub, wide), bf16),
            pltpu.VMEM((units, sub, wide), bf16),
            pltpu.VMEM((R // 2, block_units, sub, wide), bf16),
            pltpu.VMEM((2, sub, wide), f32),
            pltpu.VMEM((stat_rows, cols), f32),
            pltpu.VMEM((R, stat_rows, cols), f32),
            dma((2,)),
            dma((2, units)),
            dma((units,)),
            dma((units,)),
            dma((units,)),
            dma((R // 2, block_units)),
            dma((R,)),
            dma((R,)),
        ],
        compiler_params=pltpu.CompilerParams(
            collective_id=0, has_side_effects=True, vmem_limit_bytes=VMEM_LIMIT
        ),
    )(tokens.reshape(S, sub, features), frozen_weight, at, input_factor, bp)


def reduce_kernel(axes, sizes, with_rows, *refs):
    if with_rows:
        x, rows_ref, out, rows_out, inbox, s1, r1, s2, r2, rsend, rrecv = refs
    else:
        x, out, inbox, s1, r1, s2, r2 = refs
    first, second = axes
    n1, n2 = sizes
    g = n1 * n2
    me = lax.axis_index(first) * n2 + lax.axis_index(second)

    def device(i):
        peer = (me + i) % g
        return {first: peer // n2, second: peer % n2}

    barrier = pltpu.get_barrier_semaphore()

    def loop(body):
        def step(i, carry):
            body(i)
            return carry

        lax.fori_loop(1, g, step, 0)

    loop(lambda i: pl.semaphore_signal(barrier, inc=1, device_id=device(i), device_id_type=MESH))
    pl.semaphore_wait(barrier, g - 1)

    def scatter(i):
        return pltpu.make_async_remote_copy(
            src_ref=x.at[(me + i) % g], dst_ref=inbox.at[i], send_sem=s1.at[i], recv_sem=r1.at[i],
            device_id=device(i), device_id_type=MESH,
        )

    def spread(i, piece):
        return pltpu.make_async_remote_copy(
            src_ref=out.at[piece], dst_ref=out.at[piece], send_sem=s2.at[i], recv_sem=r2.at[i],
            device_id=device(i), device_id_type=MESH,
        )

    loop(lambda i: scatter(i).start())
    if with_rows:
        mine = lax.axis_index(second)

        def row_copy(i, piece):
            return pltpu.make_async_remote_copy(
                src_ref=rows_ref, dst_ref=rows_out.at[piece], send_sem=rsend.at[i],
                recv_sem=rrecv.at[i], device_id={second: (mine + i) % n2}, device_id_type=MESH,
            )

        for i in range(1, n2):
            row_copy(i, mine).start()
        rows_out[mine] = rows_ref[...]

    def gathered(i, total):
        scatter(i).wait_recv()
        return total + inbox[i]

    out[me] = lax.fori_loop(1, g, gathered, x[me])
    loop(lambda i: spread(i, me).start())
    loop(lambda i: spread(i, (me - i + g) % g).wait_recv())
    if with_rows:
        for i in range(1, n2):
            row_copy(i, (mine - i + n2) % n2).wait_recv()
        for i in range(1, n2):
            row_copy(i, mine).wait_send()
    loop(lambda i: scatter(i).wait_send())
    loop(lambda i: spread(i, me).wait_send())


def group_sum(value, axes, identity, rows=None):
    sizes = tuple(lax.axis_size(name) for name in axes)
    g = sizes[0] * sizes[1]
    shape = value.shape
    x = value.reshape(g, -1, LANES)
    vmem = pl.BlockSpec(memory_space=pltpu.VMEM)
    dma = pltpu.SemaphoreType.DMA
    out_shape = [jax.ShapeDtypeStruct(x.shape, jnp.float32)]
    operands = [x]
    scratch = [pltpu.VMEM(x.shape, jnp.float32)] + [dma((g,))] * 4
    if rows is not None:
        out_shape.append(jax.ShapeDtypeStruct((sizes[1],) + rows.shape, jnp.float32))
        operands.append(rows)
        scratch += [dma((sizes[1],))] * 2
    results = pl.pallas_call(
        functools.partial(reduce_kernel, axes, sizes, rows is not None),
        out_shape=tuple(out_shape),
        in_specs=[vmem] * len(operands),
        out_specs=tuple([vmem] * len(out_shape)),
        scratch_shapes=scratch,
        compiler_params=pltpu.CompilerParams(collective_id=identity, has_side_effects=True),
    )(*operands)
    total = results[0].reshape(shape)
    return total if rows is None else (total, results[1])


def per_device(
    tokens,
    frozen_weight,
    input_adapter_factor,
    output_adapter_factor,
    magnitude,
    cotangent,
    sequence_lengths,
):
    row_index = lax.axis_index("row")
    group_index = lax.axis_index("dp")
    block_rows, cols = cotangent.shape
    features = tokens.shape[1]
    rank = input_adapter_factor.shape[0]
    summed, portion, stats = gather_project(
        tokens, frozen_weight, input_adapter_factor, output_adapter_factor
    )
    summed = summed.reshape(block_rows, cols + LANES)
    portion = portion.reshape(-1, features)
    merged_input_factor, norm_sq = stats[:rank], stats[rank]
    down_activations = summed[:, cols:cols + rank].astype(jnp.bfloat16)
    col_norm = jnp.sqrt(norm_sq + norm_eps)
    col_scale = magnitude / col_norm
    query_projection = summed[:, :cols] + jnp.dot(
        down_activations, output_adapter_factor, preferred_element_type=jnp.float32
    )
    projected = (query_projection * col_scale[None, :]).astype(jnp.bfloat16)
    lengths = sequence_lengths[0]
    ends = jnp.cumsum(lengths, dtype=jnp.int32)
    starts = ends - lengths
    positions = row_index * block_rows + jnp.arange(block_rows, dtype=jnp.int32)
    inside = (positions[:, None] >= starts[None, :]) & (positions[:, None] < ends[None, :])
    inverse = 1.0 / lengths.astype(jnp.float32)
    weights = jnp.sum(jnp.where(inside, inverse[None, :], jnp.float32(0.0)), axis=1)
    grad_out = cotangent.astype(jnp.float32) * weights[:, None]
    scale_terms = jnp.sum(grad_out * query_projection, axis=0)
    projection_gradient = (grad_out * col_scale[None, :]).astype(jnp.bfloat16)
    bgrad_terms = contract_product(down_activations, projection_gradient, 0, 0)
    backward_terms = contract_product(output_adapter_factor, projection_gradient, 1, 1)
    terms = jnp.concatenate([bgrad_terms, jnp.pad(scale_terms[None, :], ((0, 7), (0, 0)))], axis=0)
    terms, backward_rows = group_sum(terms, ("dp", "row"), 1, backward_terms)
    bgrad_data, scale_grad = terms[:rank], terms[rank]
    grad_mag = scale_grad / col_norm
    norm_coefficient = -scale_grad * magnitude / (col_norm * col_norm * col_norm)
    grad_b = bgrad_data + merged_input_factor * norm_coefficient[None, :]
    backward = backward_rows.transpose(1, 0, 2).reshape(rank, -1).astype(jnp.bfloat16)
    row_term = jnp.dot(backward, portion, preferred_element_type=jnp.float32)
    scaled_output_factor = (
        output_adapter_factor.astype(jnp.float32) * norm_coefficient[None, :]
    ).astype(jnp.bfloat16)
    norm_term = contract_product(scaled_output_factor, frozen_weight, 1, 1) + jnp.dot(
        contract_product(scaled_output_factor, output_adapter_factor, 1, 1),
        input_adapter_factor.astype(jnp.float32),
        precision=highest_precision,
    )
    first_group = (group_index == 0).astype(jnp.float32)
    input_factor_gradient = group_sum(row_term + first_group * norm_term, ("dp", "col"), 2)
    return (projected, grad_mag, input_factor_gradient, grad_b)


def solution(mesh):
    in_specs = (
        P(("dp", "col"), "row"),
        P("row", "col"),
        P(None, "row"),
        P(None, "col"),
        P("col"),
        P(("dp", "row"), "col"),
        P("dp", None),
    )
    out_specs = (P(("dp", "row"), "col"), P("col"), P(None, "row"), P(None, "col"))
    return jax.shard_map(
        per_device, mesh=mesh, in_specs=in_specs, out_specs=out_specs, check_vma=False
    )
```

```python
import functools

import jax
import jax.numpy as jnp
from jax import lax
from jax.experimental import pallas as pl
from jax.experimental.pallas import tpu as pltpu
from jax.sharding import PartitionSpec as P

norm_eps = 1e-06
highest_precision = lax.Precision.HIGHEST
MESH = pl.DeviceIdType.MESH
LANES = 128
VMEM_LIMIT = 60 * 1024 * 1024


def contract_product(left, right, left_dim, right_dim):
    return lax.dot_general(
        left, right, (((left_dim,), (right_dim,)), ((), ())), preferred_element_type=jnp.float32
    )


def column_tiles(width, tile):
    return [(start, min(tile, width - start)) for start in range(0, width, tile)]


def adapter_kernel(
    D, C, R, S,
    tok, w_hbm, a_ref, b_ref, magnitude, cot_hbm, lengths,
    projected, grad_mag, factor_grad, grad_b,
    wx, gath, sb, pin, xin, pb, st_in, apad, bpad, acc, pg, cot, row_weight, down_all,
    scale_in, back_in, bsum, bsum_all, box1, fsum, box2,
    load_sem, gsend, grecv, ssend, precv, xrecv, stsend, strecv,
    sc_send, sc_recv, bk_send, bk_recv, r1a, r1b, r1c, r1d, r2a, r2b, r2c, r2d,
):
    z = lax.axis_index("col")
    r = lax.axis_index("row")
    d = lax.axis_index("dp")
    p, q = r // 2, r % 2
    pairs = R // 2
    sub, features = tok.shape[1], tok.shape[2]
    cols = w_hbm.shape[1]
    rank_rows = a_ref.shape[0]
    units = C * S
    block_units = units // R
    block_rows = block_units * sub
    tiles = column_tiles(cols, 512)
    feature_tiles = column_tiles(features, 512)
    f32, bf16 = jnp.float32, jnp.bfloat16

    load_w = pltpu.make_async_copy(w_hbm, wx, load_sem.at[0])
    load_c = pltpu.make_async_copy(cot_hbm, cot, load_sem.at[1])
    load_w.start()
    load_c.start()

    g1, g2 = D * R, D * C
    me1, me2 = d * R + r, d * C + z

    def device1(i):
        peer = (me1 + i) % g1
        return {"dp": peer // R, "row": peer % R}

    def device2(i):
        peer = (me2 + i) % g2
        return {"dp": peer // C, "col": peer % C}

    def loop(n, body):
        def turn(i, carry):
            body(i)
            return carry

        lax.fori_loop(1, n, turn, 0)

    barrier = pltpu.get_barrier_semaphore()
    loop(g1, lambda i: pl.semaphore_signal(barrier, inc=1, device_id=device1(i), device_id_type=MESH))
    loop(g2, lambda i: pl.semaphore_signal(barrier, inc=1, device_id=device2(i), device_id_type=MESH))
    pl.semaphore_wait(barrier, g1 + g2 - 2)

    def hop(src, u, direction):
        target = z - 1 if direction == 0 else z + 1
        return pltpu.make_async_remote_copy(
            src_ref=src, dst_ref=gath.at[u], send_sem=gsend.at[direction, u],
            recv_sem=grecv.at[u], device_id={"col": target}, device_id_type=MESH,
        )

    for s in range(S):
        @pl.when(z > 0)
        def _():
            hop(tok.at[s], z * S + s, 0).start()

        @pl.when(z < C - 1)
        def _():
            hop(tok.at[s], z * S + s, 1).start()

    a = a_ref[...]
    apad[...] = jnp.zeros_like(apad)
    bpad[...] = jnp.zeros_like(bpad)
    apad[0:rank_rows, :] = a
    bpad[0:rank_rows, :] = b_ref[...]
    position = r * block_rows + lax.broadcasted_iota(jnp.int32, (block_rows, LANES), 0)
    weights = jnp.zeros((block_rows, LANES), f32)
    start_row = 0
    for i in range(lengths.shape[1]):
        length = lengths[0, i]
        end_row = start_row + length
        inverse = 1.0 / jnp.full((1, LANES), length, jnp.int32).astype(f32)
        weights = jnp.where((position >= start_row) & (position < end_row), inverse, weights)
        start_row = end_row
    row_weight[...] = weights

    load_w.wait()
    load_c.wait()

    gram = contract_product(a, a, 1, 1)
    for start, width in tiles:
        span = pl.ds(start, width)
        st_in[r, 0:rank_rows, span] = jnp.dot(
            a, wx[:, span], preferred_element_type=f32
        ) + jnp.dot(
            gram, b_ref[:, span].astype(f32),
            precision=highest_precision, preferred_element_type=f32,
        )
        st_in[r, rank_rows:rank_rows + 8, span] = jnp.zeros((8, width), f32)
    depth = 256

    def norm_step(i, carry):
        rows = pl.ds(pl.multiple_of(i * depth, depth), depth)
        for start, width in tiles:
            span = pl.ds(start, width)
            merged = wx[rows, span].astype(f32) + contract_product(apad[:, rows], bpad[:, span], 0, 0)
            st_in[r, rank_rows:rank_rows + 1, span] += jnp.sum(merged * merged, axis=0, keepdims=True)
        return carry

    lax.fori_loop(0, features // depth, norm_step, 0)

    def stat_copy(i, piece):
        return pltpu.make_async_remote_copy(
            src_ref=st_in.at[piece], dst_ref=st_in.at[piece], send_sem=stsend.at[i],
            recv_sem=strecv.at[i], device_id={"row": (r + i) % R}, device_id_type=MESH,
        )

    near = jnp.minimum(z, C - 1 - z)

    def place(k):
        j = k - S
        both = j < 2 * near * S
        rest = j - 2 * near * S
        distance = jnp.where(both, j // (2 * S) + 1, near + 1 + rest // S)
        s = jnp.where(both, (j % (2 * S)) // 2, rest % S)
        leftward = jnp.where(both, j % 2 == 0, z > C - 1 - z)
        chunk = jnp.where(leftward, z - distance, z + distance)
        own = k < S
        return jnp.where(own, z, chunk), jnp.where(own, k, s)

    def pair_copy(u):
        return pltpu.make_async_remote_copy(
            src_ref=sb.at[u], dst_ref=pin.at[u], send_sem=ssend.at[u], recv_sem=precv.at[u],
            device_id={"row": p * 2 + (1 - q)}, device_id_type=MESH,
        )

    def far_copy(u, owner_pair):
        return pltpu.make_async_remote_copy(
            src_ref=sb.at[u], dst_ref=xin.at[p, u % block_units], send_sem=ssend.at[u],
            recv_sem=xrecv.at[p, u % block_units],
            device_id={"row": owner_pair * 2 + q}, device_id_type=MESH,
        )

    def multiply(k):
        c, s = place(k)
        u = c * S + s
        owner = u // block_units

        @pl.when(k < S)
        def _():
            gath[u] = tok[s]

        @pl.when(k >= S)
        def _():
            hop(gath.at[u], u, 0).wait_recv()

            @pl.when((c < z) & (z < C - 1))
            def _():
                hop(gath.at[u], u, 1).start()

            @pl.when((c > z) & (z > 0))
            def _():
                hop(gath.at[u], u, 0).start()

        slot = k % 2
        for start, width in tiles:
            span = pl.ds(start, width)
            pb[slot, :, span] = jnp.dot(gath[u], wx[:, span], preferred_element_type=f32)
        pb[slot, :, pl.ds(cols, LANES)] = contract_product(gath[u], apad[...], 1, 1)

        @pl.when(owner % 2 != q)
        def _():
            sb[u] = pb[slot].astype(bf16)
            pair_copy(u).start()

    def combine(k):
        c, s = place(k)
        u = c * S + s
        owner = u // block_units
        slot = k % 2

        @pl.when(owner % 2 == q)
        def _():
            pair_copy(u).wait_recv()
            total = pb[slot] + pin[u].astype(f32)

            @pl.when(owner // 2 == p)
            def _():
                acc[u % block_units] = total

            @pl.when(owner // 2 != p)
            def _():
                sb[u] = total.astype(bf16)
                far_copy(u, owner // 2).start()

    def step(k, carry):
        @pl.when(k < units)
        def _():
            multiply(k)

        @pl.when(k == 0)
        def _():
            for i in range(1, R):
                stat_copy(i, r).start()

        @pl.when(k > 0)
        def _():
            combine(k - 1)

        return carry

    lax.fori_loop(0, units + 1, step, 0)

    for i in range(1, R):
        stat_copy(i, (r - i + R) % R).wait_recv()
    stats = st_in[0]
    for i in range(1, R):
        stats = stats + st_in[i]
    merged_factor = stats[0:rank_rows]
    col_norm = jnp.sqrt(stats[rank_rows:rank_rows + 1] + norm_eps)
    col_scale = magnitude[...] / col_norm
    scale_in[me1] = jnp.zeros((1, cols), f32)

    def finish(v, carry):
        for i in range(1, pairs):
            other = (p + i) % pairs
            pltpu.make_async_remote_copy(
                src_ref=sb.at[v], dst_ref=xin.at[other, v], send_sem=ssend.at[v],
                recv_sem=xrecv.at[other, v], device_id={"row": other * 2 + q}, device_id_type=MESH,
            ).wait_recv()
            acc[v] += xin[other, v].astype(f32)
        rows = pl.ds(pl.multiple_of(v * sub, sub), sub)
        down = acc[v, :, pl.ds(cols, LANES)].astype(bf16)
        down_all[rows, :] = down
        weight = row_weight[rows, 0:1]
        for start, width in tiles:
            span = pl.ds(start, width)
            scale = col_scale[:, start:start + width]
            query = acc[v, :, span] + jnp.dot(down, bpad[:, span], preferred_element_type=f32)
            projected[rows, span] = (query * scale).astype(bf16)
            grad_out = cot[rows, span].astype(f32) * weight
            scale_in[me1, :, span] += jnp.sum(grad_out * query, axis=0, keepdims=True)
            pg[rows, span] = (grad_out * scale).astype(bf16)
        return carry

    lax.fori_loop(0, block_units, finish, 0)

    def scale_copy(i, piece):
        return pltpu.make_async_remote_copy(
            src_ref=scale_in.at[piece], dst_ref=scale_in.at[piece], send_sem=sc_send.at[i],
            recv_sem=sc_recv.at[i], device_id=device1(i), device_id_type=MESH,
        )

    def back_copy(i, piece):
        return pltpu.make_async_remote_copy(
            src_ref=back_in.at[piece], dst_ref=back_in.at[piece], send_sem=bk_send.at[i],
            recv_sem=bk_recv.at[i], device_id={"row": (r + i) % R}, device_id_type=MESH,
        )

    back_in[r] = contract_product(b_ref[...], pg[...], 1, 1).astype(bf16)
    loop(g1, lambda i: scale_copy(i, me1).start())
    for i in range(1, R):
        back_copy(i, r).start()

    def group_sum(g, me, device, src, box, out, s1, r1, s2, r2):
        width = max(LANES, src.shape[1] // g)
        pieces = src.shape[1] // width

        def part(j):
            return pl.ds(pl.multiple_of(j * width, width), width)

        def scatter(i):
            return pltpu.make_async_remote_copy(
                src_ref=src.at[:, part((me + i) % g % pieces)], dst_ref=box.at[i],
                send_sem=s1.at[i], recv_sem=r1.at[i], device_id=device(i), device_id_type=MESH,
            )

        def spread(i, j):
            return pltpu.make_async_remote_copy(
                src_ref=out.at[:, part(j % pieces)], dst_ref=out.at[:, part(j % pieces)],
                send_sem=s2.at[i], recv_sem=r2.at[i], device_id=device(i), device_id_type=MESH,
            )

        def to_owner(i, action):
            @pl.when((me + i) % g < pieces)
            def _():
                action(scatter(i))

        def from_owner(i, action):
            @pl.when((me - i + g) % g < pieces)
            def _():
                action(spread(i, (me - i + g) % g))

        def begin():
            loop(g, lambda i: to_owner(i, lambda copy: copy.start()))

        def middle():
            @pl.when(me < pieces)
            def _():
                def add(i, total):
                    scatter(i).wait_recv()
                    return total + box[i]

                out[:, part(me % pieces)] = lax.fori_loop(1, g, add, src[:, part(me % pieces)])
                loop(g, lambda i: spread(i, me).start())

        def end():
            loop(g, lambda i: from_owner(i, lambda copy: copy.wait_recv()))

        def drain():
            loop(g, lambda i: to_owner(i, lambda copy: copy.wait_send()))

            @pl.when(me < pieces)
            def _():
                loop(g, lambda i: spread(i, me).wait_send())

        return begin, middle, end, drain

    begin1, middle1, end1, drain1 = group_sum(
        g1, me1, device1, bsum, box1, bsum_all, r1a, r1b, r1c, r1d
    )
    begin2, middle2, end2, drain2 = group_sum(
        g2, me2, device2, fsum, box2, factor_grad, r2a, r2b, r2c, r2d
    )
    for start, width in tiles:
        span = pl.ds(start, width)
        bsum[:, span] = contract_product(down_all[...], pg[:, span], 0, 0)[0:rank_rows]
    begin1()

    for i in range(1, R):
        back_copy(i, (r - i + R) % R).wait_recv()
    for start, width in feature_tiles:
        span = pl.ds(start, width)
        term = jnp.zeros((rank_rows, width), f32)
        for j in range(R):
            block = gath[j * block_units:(j + 1) * block_units, :, span].reshape(block_rows, width)
            term = term + jnp.dot(back_in[j], block, preferred_element_type=f32)
        fsum[:, span] = term

    loop(g1, lambda i: scale_copy(i, (me1 - i + g1) % g1).wait_recv())
    scale_grad = scale_in[0]
    for j in range(1, g1):
        scale_grad = scale_grad + scale_in[j]
    grad_mag[...] = scale_grad / col_norm
    coefficient = -scale_grad * magnitude[...] / (col_norm * col_norm * col_norm)
    scaled = (b_ref[...].astype(f32) * coefficient).astype(bf16)
    cross = contract_product(scaled, b_ref[...], 1, 1)
    for index, (start, width) in enumerate(feature_tiles):
        @pl.when(d == index % D)
        def _():
            span = pl.ds(start, width)
            fsum[:, span] += contract_product(scaled, wx[span, :], 1, 1) + jnp.dot(
                cross, a_ref[:, span].astype(f32),
                precision=highest_precision, preferred_element_type=f32,
            )
    begin2()
    middle1()
    middle2()
    end1()
    grad_b[...] = bsum_all[...] + merged_factor * coefficient
    end2()

    drain1()
    drain2()
    loop(g1, lambda i: scale_copy(i, me1).wait_send())
    for i in range(1, R):
        stat_copy(i, r).wait_send()
        back_copy(i, r).wait_send()

    def drain(u, carry):
        c = u // S
        owner = u // block_units

        @pl.when((owner % 2 != q) | (owner // 2 != p))
        def _():
            pair_copy(u).wait_send()

        @pl.when((c <= z) & (z < C - 1))
        def _():
            hop(gath.at[u], u, 1).wait_send()

        @pl.when((c >= z) & (z > 0))
        def _():
            hop(gath.at[u], u, 0).wait_send()

        return carry

    lax.fori_loop(0, units, drain, 0)


def per_device(
    tokens,
    frozen_weight,
    input_adapter_factor,
    output_adapter_factor,
    magnitude,
    cotangent,
    sequence_lengths,
):
    D, C, R = lax.axis_size("dp"), lax.axis_size("col"), lax.axis_size("row")
    local_rows, features = tokens.shape
    block_rows, cols = cotangent.shape
    rank_rows = input_adapter_factor.shape[0]
    S = 4
    sub = local_rows // S
    units = C * S
    block_units = units // R
    wide = cols + LANES
    g1, g2 = D * R, D * C
    vmem = pl.BlockSpec(memory_space=pltpu.VMEM)
    smem = pl.BlockSpec(memory_space=pltpu.SMEM)
    hbm = pl.BlockSpec(memory_space=pl.ANY)
    dma = pltpu.SemaphoreType.DMA
    f32, bf16 = jnp.float32, jnp.bfloat16
    projected, grad_mag, factor_grad, grad_b = pl.pallas_call(
        functools.partial(adapter_kernel, D, C, R, S),
        out_shape=(
            jax.ShapeDtypeStruct((block_rows, cols), bf16),
            jax.ShapeDtypeStruct((1, cols), f32),
            jax.ShapeDtypeStruct((rank_rows, features), f32),
            jax.ShapeDtypeStruct((rank_rows, cols), f32),
        ),
        in_specs=[vmem, hbm, vmem, vmem, vmem, hbm, smem],
        out_specs=(vmem, vmem, vmem, vmem),
        scratch_shapes=[
            pltpu.VMEM((features, cols), bf16),
            pltpu.VMEM((units, sub, features), bf16),
            pltpu.VMEM((units, sub, wide), bf16),
            pltpu.VMEM((units, sub, wide), bf16),
            pltpu.VMEM((R // 2, block_units, sub, wide), bf16),
            pltpu.VMEM((2, sub, wide), f32),
            pltpu.VMEM((R, rank_rows + 8, cols), f32),
            pltpu.VMEM((LANES, features), bf16),
            pltpu.VMEM((LANES, cols), bf16),
            pltpu.VMEM((block_units, sub, wide), f32),
            pltpu.VMEM((block_rows, cols), bf16),
            pltpu.VMEM((block_rows, cols), bf16),
            pltpu.VMEM((block_rows, LANES), f32),
            pltpu.VMEM((block_rows, LANES), bf16),
            pltpu.VMEM((g1, 1, cols), f32),
            pltpu.VMEM((R, rank_rows, block_rows), bf16),
            pltpu.VMEM((rank_rows, cols), f32),
            pltpu.VMEM((rank_rows, cols), f32),
            pltpu.VMEM((g1, rank_rows, max(LANES, cols // g1)), f32),
            pltpu.VMEM((rank_rows, features), f32),
            pltpu.VMEM((g2, rank_rows, max(LANES, features // g2)), f32),
            dma((2,)),
            dma((2, units)),
            dma((units,)),
            dma((units,)),
            dma((units,)),
            dma((R // 2, block_units)),
            dma((R,)),
            dma((R,)),
            dma((g1,)),
            dma((g1,)),
            dma((R,)),
            dma((R,)),
        ] + [dma((g1,))] * 4 + [dma((g2,))] * 4,
        compiler_params=pltpu.CompilerParams(
            collective_id=0, has_side_effects=True, vmem_limit_bytes=VMEM_LIMIT
        ),
    )(
        tokens.reshape(S, sub, features), frozen_weight, input_adapter_factor,
        output_adapter_factor, magnitude.reshape(1, cols), cotangent, sequence_lengths,
    )
    return projected, grad_mag.reshape(cols), factor_grad, grad_b


def solution(mesh):
    in_specs = (
        P(("dp", "col"), "row"),
        P("row", "col"),
        P(None, "row"),
        P(None, "col"),
        P("col"),
        P(("dp", "row"), "col"),
        P("dp", None),
    )
    out_specs = (P(("dp", "row"), "col"), P("col"), P(None, "row"), P(None, "col"))
    return jax.shard_map(
        per_device, mesh=mesh, in_specs=in_specs, out_specs=out_specs, check_vma=False
    )
```

```python
import functools

import jax
import jax.numpy as jnp
from jax import lax
from jax.experimental import pallas as pl
from jax.experimental.pallas import tpu as pltpu
from jax.sharding import PartitionSpec as P

norm_eps = 1e-06
highest_precision = lax.Precision.HIGHEST
MESH = pl.DeviceIdType.MESH
LANES = 128
VMEM_LIMIT = 60 * 1024 * 1024


def contract_product(left, right, left_dim, right_dim):
    return lax.dot_general(
        left, right, (((left_dim,), (right_dim,)), ((), ())), preferred_element_type=jnp.float32
    )


def column_tiles(width, tile):
    return [(start, min(tile, width - start)) for start in range(0, width, tile)]


def adapter_kernel(
    D, C, R, S,
    tok, w_hbm, a_ref, b_ref, magnitude, cot_hbm, lengths,
    projected_hbm, grad_mag, factor_grad, grad_b,
    projected, norm_row, scale_row, fsum_all, wx, gath, sb, pin, xin, pb, st_in, apad, bpad, acc, pg, cot, row_weight, down_all,
    scale_in, back_in, bsum, bsum_all, box1, fsum, box2,
    load_sem, gsend, grecv, ssend, precv, xrecv, stsend, strecv,
    sc_send, sc_recv, bk_send, bk_recv, r1a, r1b, r1c, r1d, r2a, r2b, r2c, r2d,
):
    z = lax.axis_index("col")
    r = lax.axis_index("row")
    d = lax.axis_index("dp")
    p, q = r // 2, r % 2
    pairs = R // 2
    sub, features = tok.shape[1], tok.shape[2]
    cols = w_hbm.shape[1]
    rank_rows = a_ref.shape[0]
    units = C * S
    block_units = units // R
    block_rows = block_units * sub
    tiles = column_tiles(cols, 512)
    feature_tiles = column_tiles(features, 512)
    f32, bf16 = jnp.float32, jnp.bfloat16

    load_w = pltpu.make_async_copy(w_hbm, wx, load_sem.at[0])
    load_c = pltpu.make_async_copy(cot_hbm, cot, load_sem.at[1])
    load_w.start()
    load_c.start()

    g1, g2 = D * R, D * C
    me1, me2 = d * R + r, d * C + z

    def device1(i):
        peer = (me1 + i) % g1
        return {"dp": peer // R, "row": peer % R}

    def device2(i):
        peer = (me2 + i) % g2
        return {"dp": peer // C, "col": peer % C}

    def loop(n, body):
        def turn(i, carry):
            body(i)
            return carry

        lax.fori_loop(1, n, turn, 0)

    barrier = pltpu.get_barrier_semaphore()
    loop(g1, lambda i: pl.semaphore_signal(barrier, inc=1, device_id=device1(i), device_id_type=MESH))
    loop(g2, lambda i: pl.semaphore_signal(barrier, inc=1, device_id=device2(i), device_id_type=MESH))
    pl.semaphore_wait(barrier, g1 + g2 - 2)

    def hop(src, u, direction):
        target = z - 1 if direction == 0 else z + 1
        return pltpu.make_async_remote_copy(
            src_ref=src, dst_ref=gath.at[u], send_sem=gsend.at[direction, u],
            recv_sem=grecv.at[u], device_id={"col": target}, device_id_type=MESH,
        )

    for s in range(S):
        @pl.when(z > 0)
        def _():
            hop(tok.at[s], z * S + s, 0).start()

        @pl.when(z < C - 1)
        def _():
            hop(tok.at[s], z * S + s, 1).start()

    a = a_ref[...]
    apad[...] = jnp.zeros_like(apad)
    bpad[...] = jnp.zeros_like(bpad)
    apad[0:rank_rows, :] = a
    bpad[0:rank_rows, :] = b_ref[...]
    position = r * block_rows + lax.broadcasted_iota(jnp.int32, (block_rows, LANES), 0)
    weights = jnp.zeros((block_rows, LANES), f32)
    start_row = 0
    for i in range(lengths.shape[1]):
        length = lengths[0, i]
        end_row = start_row + length
        inverse = 1.0 / jnp.full((1, LANES), length, jnp.int32).astype(f32)
        weights = jnp.where((position >= start_row) & (position < end_row), inverse, weights)
        start_row = end_row
    row_weight[...] = weights

    load_w.wait()
    load_c.wait()

    gram = contract_product(a, a, 1, 1)
    for start, width in tiles:
        span = pl.ds(start, width)
        st_in[r, 0:rank_rows, span] = jnp.dot(
            a, wx[:, span], preferred_element_type=f32
        ) + jnp.dot(
            gram, b_ref[:, span].astype(f32),
            precision=highest_precision, preferred_element_type=f32,
        )
        st_in[r, rank_rows:rank_rows + 8, span] = jnp.zeros((8, width), f32)
    depth = 256

    def norm_step(i, carry):
        rows = pl.ds(pl.multiple_of(i * depth, depth), depth)
        for start, width in tiles:
            span = pl.ds(start, width)
            merged = wx[rows, span].astype(f32) + contract_product(apad[:, rows], bpad[:, span], 0, 0)
            st_in[r, rank_rows:rank_rows + 1, span] += jnp.sum(merged * merged, axis=0, keepdims=True)
        return carry

    lax.fori_loop(0, features // depth, norm_step, 0)

    def stat_copy(i, piece):
        return pltpu.make_async_remote_copy(
            src_ref=st_in.at[piece], dst_ref=st_in.at[piece], send_sem=stsend.at[i],
            recv_sem=strecv.at[i], device_id={"row": (r + i) % R}, device_id_type=MESH,
        )

    near = jnp.minimum(z, C - 1 - z)

    def place(k):
        j = k - S
        both = j < 2 * near * S
        rest = j - 2 * near * S
        distance = jnp.where(both, j // (2 * S) + 1, near + 1 + rest // S)
        s = jnp.where(both, (j % (2 * S)) // 2, rest % S)
        leftward = jnp.where(both, j % 2 == 0, z > C - 1 - z)
        chunk = jnp.where(leftward, z - distance, z + distance)
        own = k < S
        return jnp.where(own, z, chunk), jnp.where(own, k, s)

    def pair_copy(u):
        return pltpu.make_async_remote_copy(
            src_ref=sb.at[u], dst_ref=pin.at[u], send_sem=ssend.at[u], recv_sem=precv.at[u],
            device_id={"row": p * 2 + (1 - q)}, device_id_type=MESH,
        )

    def far_copy(u, owner_pair):
        return pltpu.make_async_remote_copy(
            src_ref=sb.at[u], dst_ref=xin.at[p, u % block_units], send_sem=ssend.at[u],
            recv_sem=xrecv.at[p, u % block_units],
            device_id={"row": owner_pair * 2 + q}, device_id_type=MESH,
        )

    def multiply(k):
        c, s = place(k)
        u = c * S + s
        owner = u // block_units

        @pl.when(k < S)
        def _():
            gath[u] = tok[s]

        @pl.when(k >= S)
        def _():
            hop(gath.at[u], u, 0).wait_recv()

            @pl.when((c < z) & (z < C - 1))
            def _():
                hop(gath.at[u], u, 1).start()

            @pl.when((c > z) & (z > 0))
            def _():
                hop(gath.at[u], u, 0).start()

        slot = k % 2
        for start, width in tiles:
            span = pl.ds(start, width)
            pb[slot, :, span] = jnp.dot(gath[u], wx[:, span], preferred_element_type=f32)
        pb[slot, :, pl.ds(cols, LANES)] = contract_product(gath[u], apad[...], 1, 1)

        @pl.when(owner % 2 != q)
        def _():
            sb[u] = pb[slot].astype(bf16)
            pair_copy(u).start()

    def combine(k):
        c, s = place(k)
        u = c * S + s
        owner = u // block_units
        slot = k % 2

        @pl.when(owner % 2 == q)
        def _():
            pair_copy(u).wait_recv()
            total = pb[slot] + pin[u].astype(f32)

            @pl.when(owner // 2 == p)
            def _():
                acc[u % block_units] = total

            @pl.when(owner // 2 != p)
            def _():
                sb[u] = total.astype(bf16)
                far_copy(u, owner // 2).start()

    scale_in[me1] = jnp.zeros((1, cols), f32)

    def prepare():
        for i in range(1, R):
            stat_copy(i, (r - i + R) % R).wait_recv()
        norm_sq = st_in[0, rank_rows:rank_rows + 1]
        for i in range(1, R):
            norm_sq = norm_sq + st_in[i, rank_rows:rank_rows + 1]
        norm = jnp.sqrt(norm_sq + norm_eps)
        norm_row[...] = norm
        scale_row[...] = magnitude[...] / norm

    def finish(v):
        for i in range(1, pairs):
            other = (p + i) % pairs
            pltpu.make_async_remote_copy(
                src_ref=sb.at[v], dst_ref=xin.at[other, v], send_sem=ssend.at[v],
                recv_sem=xrecv.at[other, v], device_id={"row": other * 2 + q}, device_id_type=MESH,
            ).wait_recv()
            acc[v] += xin[other, v].astype(f32)
        rows = pl.ds(pl.multiple_of(v * sub, sub), sub)
        down = acc[v, :, pl.ds(cols, LANES)].astype(bf16)
        down_all[rows, :] = down
        weight = row_weight[rows, 0:1]
        for start, width in tiles:
            span = pl.ds(start, width)
            scale = scale_row[:, span]
            query = acc[v, :, span] + jnp.dot(down, bpad[:, span], preferred_element_type=f32)
            projected[rows, span] = (query * scale).astype(bf16)
            grad_out = cot[rows, span].astype(f32) * weight
            scale_in[me1, :, span] += jnp.sum(grad_out * query, axis=0, keepdims=True)
            pg[rows, span] = (grad_out * scale).astype(bf16)

    lag = min(3, units)

    def step(k, carry):
        @pl.when(k < units)
        def _():
            multiply(k)

        @pl.when(k == 0)
        def _():
            for i in range(1, R):
                stat_copy(i, r).start()

        @pl.when((k > 0) & (k <= units))
        def _():
            combine(k - 1)

        @pl.when(k == lag)
        def _():
            prepare()

        @pl.when(k >= lag)
        def _():
            c, s = place(k - lag)
            u = c * S + s

            @pl.when(u // block_units == r)
            def _():
                finish(u % block_units)

        return carry

    lax.fori_loop(0, units + lag, step, 0)
    leave = pltpu.make_async_copy(projected, projected_hbm, load_sem.at[0])
    leave.start()
    col_norm = norm_row[...]
    merged_factor = st_in[0, 0:rank_rows]
    for i in range(1, R):
        merged_factor = merged_factor + st_in[i, 0:rank_rows]

    def scale_copy(i, piece):
        return pltpu.make_async_remote_copy(
            src_ref=scale_in.at[piece], dst_ref=scale_in.at[piece], send_sem=sc_send.at[i],
            recv_sem=sc_recv.at[i], device_id=device1(i), device_id_type=MESH,
        )

    def back_copy(i, piece):
        return pltpu.make_async_remote_copy(
            src_ref=back_in.at[piece], dst_ref=back_in.at[piece], send_sem=bk_send.at[i],
            recv_sem=bk_recv.at[i], device_id={"row": (r + i) % R}, device_id_type=MESH,
        )

    back_in[r] = contract_product(b_ref[...], pg[...], 1, 1).astype(bf16)
    loop(g1, lambda i: scale_copy(i, me1).start())
    for i in range(1, R):
        back_copy(i, r).start()

    def group_sum(g, me, device, src, box, out, s1, r1, s2, r2):
        width = max(LANES, src.shape[1] // g)
        pieces = src.shape[1] // width

        def part(j):
            return pl.ds(pl.multiple_of(j * width, width), width)

        def scatter(i):
            return pltpu.make_async_remote_copy(
                src_ref=src.at[:, part((me + i) % g % pieces)], dst_ref=box.at[i],
                send_sem=s1.at[i], recv_sem=r1.at[i], device_id=device(i), device_id_type=MESH,
            )

        def spread(i, j):
            return pltpu.make_async_remote_copy(
                src_ref=out.at[:, part(j % pieces)], dst_ref=out.at[:, part(j % pieces)],
                send_sem=s2.at[i], recv_sem=r2.at[i], device_id=device(i), device_id_type=MESH,
            )

        def to_owner(i, action):
            @pl.when((me + i) % g < pieces)
            def _():
                action(scatter(i))

        def from_owner(i, action):
            @pl.when((me - i + g) % g < pieces)
            def _():
                action(spread(i, (me - i + g) % g))

        def begin():
            loop(g, lambda i: to_owner(i, lambda copy: copy.start()))

        def middle():
            @pl.when(me < pieces)
            def _():
                def add(i, total):
                    scatter(i).wait_recv()
                    return total + box[i]

                total = lax.fori_loop(1, g, add, src[:, part(me % pieces)])
                out[:, part(me % pieces)] = total.astype(out.dtype)
                loop(g, lambda i: spread(i, me).start())

        def end():
            loop(g, lambda i: from_owner(i, lambda copy: copy.wait_recv()))

        def drain():
            loop(g, lambda i: to_owner(i, lambda copy: copy.wait_send()))

            @pl.when(me < pieces)
            def _():
                loop(g, lambda i: spread(i, me).wait_send())

        return begin, middle, end, drain

    begin1, middle1, end1, drain1 = group_sum(
        g1, me1, device1, bsum, box1, bsum_all, r1a, r1b, r1c, r1d
    )
    begin2, middle2, end2, drain2 = group_sum(
        g2, me2, device2, fsum, box2, fsum_all, r2a, r2b, r2c, r2d
    )
    for start, width in tiles:
        span = pl.ds(start, width)
        bsum[:, span] = contract_product(down_all[...], pg[:, span], 0, 0)[0:rank_rows]
    begin1()

    for i in range(1, R):
        back_copy(i, (r - i + R) % R).wait_recv()
    for start, width in feature_tiles:
        span = pl.ds(start, width)
        term = jnp.zeros((rank_rows, width), f32)
        for j in range(R):
            block = gath[j * block_units:(j + 1) * block_units, :, span].reshape(block_rows, width)
            term = term + jnp.dot(back_in[j], block, preferred_element_type=f32)
        fsum[:, span] = term

    loop(g1, lambda i: scale_copy(i, (me1 - i + g1) % g1).wait_recv())
    scale_grad = scale_in[0]
    for j in range(1, g1):
        scale_grad = scale_grad + scale_in[j]
    grad_mag[...] = scale_grad / col_norm
    coefficient = -scale_grad * magnitude[...] / (col_norm * col_norm * col_norm)
    scaled = (b_ref[...].astype(f32) * coefficient).astype(bf16)
    cross = contract_product(scaled, b_ref[...], 1, 1)
    for index, (start, width) in enumerate(feature_tiles):
        @pl.when(d == index % D)
        def _():
            span = pl.ds(start, width)
            fsum[:, span] += contract_product(scaled, wx[span, :], 1, 1) + jnp.dot(
                cross, a_ref[:, span].astype(f32),
                precision=highest_precision, preferred_element_type=f32,
            )
    begin2()
    middle1()
    middle2()
    end1()
    grad_b[...] = bsum_all[...] + merged_factor * coefficient
    end2()
    factor_grad[...] = fsum_all[...].astype(f32)
    leave.wait()

    drain1()
    drain2()
    loop(g1, lambda i: scale_copy(i, me1).wait_send())
    for i in range(1, R):
        stat_copy(i, r).wait_send()
        back_copy(i, r).wait_send()

    def drain(u, carry):
        c = u // S
        owner = u // block_units

        @pl.when((owner % 2 != q) | (owner // 2 != p))
        def _():
            pair_copy(u).wait_send()

        @pl.when((c <= z) & (z < C - 1))
        def _():
            hop(gath.at[u], u, 1).wait_send()

        @pl.when((c >= z) & (z > 0))
        def _():
            hop(gath.at[u], u, 0).wait_send()

        return carry

    lax.fori_loop(0, units, drain, 0)


def deliver_kernel(*refs):
    sources, targets, held, loaded, stored = refs[:4], refs[4:8], refs[8:12], refs[12], refs[13]
    loads = [pltpu.make_async_copy(sources[i], held[i], loaded.at[i]) for i in range(4)]
    stores = [pltpu.make_async_copy(held[i], targets[i], stored.at[i]) for i in range(4)]
    for load in loads:
        load.start()
    for load, store in zip(loads, stores):
        load.wait()
        store.start()
    for store in stores:
        store.wait()


def per_device(
    tokens,
    frozen_weight,
    input_adapter_factor,
    output_adapter_factor,
    magnitude,
    cotangent,
    sequence_lengths,
):
    D, C, R = lax.axis_size("dp"), lax.axis_size("col"), lax.axis_size("row")
    local_rows, features = tokens.shape
    block_rows, cols = cotangent.shape
    rank_rows = input_adapter_factor.shape[0]
    S = 4
    sub = local_rows // S
    units = C * S
    block_units = units // R
    wide = cols + LANES
    g1, g2 = D * R, D * C
    vmem = pl.BlockSpec(memory_space=pltpu.VMEM)
    smem = pl.BlockSpec(memory_space=pltpu.SMEM)
    hbm = pl.BlockSpec(memory_space=pl.ANY)
    dma = pltpu.SemaphoreType.DMA
    f32, bf16 = jnp.float32, jnp.bfloat16
    projected, grad_mag, factor_grad, grad_b = pl.pallas_call(
        functools.partial(adapter_kernel, D, C, R, S),
        out_shape=(
            jax.ShapeDtypeStruct((block_rows, cols), bf16),
            jax.ShapeDtypeStruct((1, cols), f32),
            jax.ShapeDtypeStruct((rank_rows, features), f32),
            jax.ShapeDtypeStruct((rank_rows, cols), f32),
        ),
        in_specs=[vmem, hbm, vmem, vmem, vmem, hbm, smem],
        out_specs=(hbm, vmem, vmem, vmem),
        scratch_shapes=[
            pltpu.VMEM((block_rows, cols), bf16),
            pltpu.VMEM((1, cols), f32),
            pltpu.VMEM((1, cols), f32),
            pltpu.VMEM((rank_rows, features), bf16),
            pltpu.VMEM((features, cols), bf16),
            pltpu.VMEM((units, sub, features), bf16),
            pltpu.VMEM((units, sub, wide), bf16),
            pltpu.VMEM((units, sub, wide), bf16),
            pltpu.VMEM((R // 2, block_units, sub, wide), bf16),
            pltpu.VMEM((2, sub, wide), f32),
            pltpu.VMEM((R, rank_rows + 8, cols), f32),
            pltpu.VMEM((LANES, features), bf16),
            pltpu.VMEM((LANES, cols), bf16),
            pltpu.VMEM((block_units, sub, wide), f32),
            pltpu.VMEM((block_rows, cols), bf16),
            pltpu.VMEM((block_rows, cols), bf16),
            pltpu.VMEM((block_rows, LANES), f32),
            pltpu.VMEM((block_rows, LANES), bf16),
            pltpu.VMEM((g1, 1, cols), f32),
            pltpu.VMEM((R, rank_rows, block_rows), bf16),
            pltpu.VMEM((rank_rows, cols), f32),
            pltpu.VMEM((rank_rows, cols), f32),
            pltpu.VMEM((g1, rank_rows, max(LANES, cols // g1)), f32),
            pltpu.VMEM((rank_rows, features), f32),
            pltpu.VMEM((g2, rank_rows, max(LANES, features // g2)), f32),
            dma((2,)),
            dma((2, units)),
            dma((units,)),
            dma((units,)),
            dma((units,)),
            dma((R // 2, block_units)),
            dma((R,)),
            dma((R,)),
            dma((g1,)),
            dma((g1,)),
            dma((R,)),
            dma((R,)),
        ] + [dma((g1,))] * 4 + [dma((g2,))] * 4,
        compiler_params=pltpu.CompilerParams(
            collective_id=0, has_side_effects=True, vmem_limit_bytes=VMEM_LIMIT
        ),
    )(
        tokens.reshape(S, sub, features), frozen_weight, input_adapter_factor,
        output_adapter_factor, magnitude.reshape(1, cols), cotangent, sequence_lengths,
    )
    projected, grad_mag, factor_grad, grad_b = pl.pallas_call(
        deliver_kernel,
        out_shape=tuple(
            jax.ShapeDtypeStruct(x.shape, x.dtype) for x in (projected, grad_mag, factor_grad, grad_b)
        ),
        in_specs=[hbm] * 4,
        out_specs=(hbm,) * 4,
        scratch_shapes=[
            pltpu.VMEM(x.shape, x.dtype) for x in (projected, grad_mag, factor_grad, grad_b)
        ] + [dma((4,)), dma((4,))],
    )(projected, grad_mag, factor_grad, grad_b)
    return projected, grad_mag.reshape(cols), factor_grad, grad_b


def solution(mesh):
    in_specs = (
        P(("dp", "col"), "row"),
        P("row", "col"),
        P(None, "row"),
        P(None, "col"),
        P("col"),
        P(("dp", "row"), "col"),
        P("dp", None),
    )
    out_specs = (P(("dp", "row"), "col"), P("col"), P(None, "row"), P(None, "col"))
    return jax.shard_map(
        per_device, mesh=mesh, in_specs=in_specs, out_specs=out_specs, check_vma=False
    )
```
